16 devices in a mesh: rep: 4 (over y, z, core), pp: 4 (over x).
Axes of the slice: x: 4, y: 2, z: 1, core: 2. Of those that a mesh axis runs over, the one named last changes fastest.
The devices are a block of a 4x4x8 slice.
Arguments:
- x: bfloat16 [32, 512, 512], P('rep'), parts along dimension 0
- dy: bfloat16 [32, 512, 512], P('rep'), parts along dimension 0
- w_gate: bfloat16 [4, 512, 1408], P('pp')
- w_up: bfloat16 [4, 512, 1408], P('pp')
- w_down: bfloat16 [4, 1408, 512], P('pp')
Outputs:
- output 1: bfloat16 [16, 512, 1408], P(('rep', 'pp')), parts along dimension 0
- output 2: bfloat16 [16, 512, 1408], P(('rep', 'pp')), parts along dimension 0
- output 3: bfloat16 [16, 1408, 512], P(('rep', 'pp')), parts along dimension 0
There are 4 independent parts. The reference program is written for one: setup_inputs(seed, part) draws one part's arguments, and reference() takes and returns one part's arrays. A program takes and returns all parts, laid end to end along the dimension named above; an argument that names none is the same for every part.
All inputs are finite; a program needn't handle non-finite values.
Results may differ from the reference program's by a relative error of at most 0.018.
Values are sent between devices in bfloat16 or wider.
A program may use at most 768 MiB of HBM per device.

```python
import jax
import jax.numpy as jnp
from jax import lax

MICRO = 8
TOKENS = 512
D = 512
FF = 1408
LAYERS = 4
NAMES = ("w_gate", "w_up", "w_down")
SHAPES = {"w_gate": (LAYERS, D, FF), "w_up": (LAYERS, D, FF), "w_down": (LAYERS, FF, D)}


def bump(key, n, height):
    away = (jnp.arange(n, dtype=jnp.int32) - jax.random.randint(key, (), 0, n, jnp.int32)) % n
    return jnp.where(away < n // 8, height, 1.0)


def together(key, own, strength):
    shared = jax.random.normal(key, own.shape[1:], jnp.float32)
    return (own + strength * shared) * lax.rsqrt(1 + strength * strength)


def setup_inputs(seed: int = 0, part: int = 0) -> dict:
    kx, kdy, ka, kb, kz, kf, kh, kl, *kw = jax.random.split(jax.random.key(seed), 8 + len(NAMES))
    kx, kdy, ka, kb = (jax.random.fold_in(k, part) for k in (kx, kdy, ka, kb))
    shape = (MICRO, TOKENS, D)
    much_x, much_dy = jax.random.uniform(kz, (2,), jnp.float32, 0.0, 1.0)
    layers = 2.0 ** jax.random.uniform(kl, (LAYERS, 1, 1), jnp.float32, -1.0, 1.0)
    x = together(ka, jax.random.normal(kx, shape, jnp.float32), much_x) * bump(kf, D, 4.0)
    dy = together(kb, jax.random.normal(kdy, shape, jnp.float32), much_dy)
    drawn = {"x": x.astype(jnp.bfloat16), "dy": (dy * (MICRO * TOKENS) ** -0.5).astype(jnp.bfloat16)}
    for key, name in zip(kw, NAMES, strict=True):
        w = jax.random.normal(key, SHAPES[name], jnp.float32) * SHAPES[name][1] ** -0.5
        drawn[name] = (w * {"w_gate": 1.0, "w_up": bump(kh, FF, 4.0), "w_down": layers}[name]).astype(jnp.bfloat16)
    return drawn


def matmul(a, w):
    return jnp.dot(a, w, preferred_element_type=jnp.float32).astype(jnp.bfloat16)


def normed(h):
    wide = h.astype(jnp.float32)
    scale = lax.rsqrt(jnp.mean(wide**2, -1, keepdims=True) + 1e-6)
    return (wide * scale).astype(jnp.bfloat16)


def layer(h, w):
    a = normed(h)
    gate = jnp.dot(a, w["w_gate"], preferred_element_type=jnp.float32)
    up = jnp.dot(a, w["w_up"], preferred_element_type=jnp.float32)
    return h + matmul((jax.nn.silu(gate) * up).astype(jnp.bfloat16), w["w_down"])


def stack(weights, h):
    return lax.scan(lambda h, w: (layer(h, w), None), h, weights)[0]


def reference(x, dy, w_gate, w_up, w_down):
    weights = dict(zip(NAMES, (w_gate, w_up, w_down), strict=True))

    def take(so_far, one):
        h, by_y = one
        _, back = jax.vjp(lambda w: stack(w, h), weights)
        return jax.tree.map(lambda total, term: total + term.astype(jnp.float32), so_far, back(by_y)[0]), None

    none_yet = {name: jnp.zeros(w.shape, jnp.float32) for name, w in weights.items()}
    by_weights, _ = lax.scan(take, none_yet, (x, dy))
    return tuple(by_weights[name].astype(jnp.bfloat16) for name in NAMES)
```

```python
import functools

import jax
import jax.numpy as jnp
from jax import lax
from jax.experimental import pallas as pl
from jax.experimental.pallas import tpu as pltpu
from jax.sharding import PartitionSpec as P

MESH = pl.DeviceIdType.MESH
F32, BF16 = jnp.float32, jnp.bfloat16
CHUNK = 128
LEAD = 4
OUT_SLOTS, BACK_SLOTS = 16, 8


def dot(a, b):
    return jnp.dot(a, b, preferred_element_type=F32)


def dot_tokens(a, b):
    return lax.dot_general(a, b, (((0,), (0,)), ((), ())), preferred_element_type=F32)


def rounded(v):
    return v.astype(BF16).astype(F32)


def kernel(
    n, x_ref, dy_ref, wg_ref, wu_ref, wd_ref, og_ref, ou_ref, od_ref,
    hbuf, dbuf, hout, dout, pbuf, qbuf, hid, dgu, abuf, wgu, wd, wgt, wut, wdt, accgu, accd,
    w_sem, hrecv, drecv, hsend, dsend, o_sem,
):
    micro, tokens, dim = x_ref.shape
    ff = wd_ref.shape[1]
    per = tokens // CHUNK
    chunks = micro * per
    slots, hid_micros = pbuf.shape[0], hid.shape[0]
    blocks = ff // 128
    me = lax.axis_index("pp")
    first, last = me == 0, me == n - 1
    lead = (n - 1 - me) * LEAD

    def rows_of(k):
        return k // per, pl.ds(pl.multiple_of((k % per) * CHUNK, CHUNK), CHUNK)

    def x_copy(k):
        m, rows = rows_of(k)
        return pltpu.make_async_copy(x_ref.at[m, rows], hbuf.at[m, rows], hrecv.at[k])

    def dy_copy(k):
        m, rows = rows_of(k)
        return pltpu.make_async_copy(dy_ref.at[m, rows], dbuf.at[m, rows], drecv.at[k])

    def h_copy(k):
        m, rows = rows_of(k)
        return pltpu.make_async_remote_copy(
            src_ref=hout.at[k % OUT_SLOTS], dst_ref=hbuf.at[m, rows], send_sem=hsend.at[k], recv_sem=hrecv.at[k],
            device_id={"pp": lax.rem(me + 1, n)}, device_id_type=MESH,
        )

    def d_copy(k):
        m, rows = rows_of(k)
        return pltpu.make_async_remote_copy(
            src_ref=dout.at[k % BACK_SLOTS], dst_ref=dbuf.at[m, rows], send_sem=dsend.at[k], recv_sem=drecv.at[k],
            device_id={"pp": lax.rem(me + n - 1, n)}, device_id_type=MESH,
        )

    loads = [pltpu.make_async_copy(wd_ref.at[0], wd, w_sem.at[2 * blocks])]
    for j in range(blocks):
        for i, ref in enumerate((wg_ref, wu_ref)):
            to = wgu.at[:, pl.ds(256 * j + 128 * i, 128)]
            loads.append(pltpu.make_async_copy(ref.at[0, :, pl.ds(128 * j, 128)], to, w_sem.at[2 * j + i]))

    @pl.when(first)
    def _():
        x_copy(0).start()

    for load in loads[1:] + loads[:1]:
        load.start()

    @pl.when(first)
    def _():
        @pl.loop(1, chunks)
        def _(k):
            x_copy(k).start()

    @pl.when(last)
    def _():
        @pl.loop(0, chunks)
        def _(k):
            dy_copy(k).start()

    barrier = pltpu.get_barrier_semaphore()

    @pl.when(me > 0)
    def _():
        pl.semaphore_signal(barrier, inc=1, device_id={"pp": lax.rem(me + n - 1, n)}, device_id_type=MESH)

    @pl.when(me < n - 1)
    def _():
        pl.semaphore_signal(barrier, inc=1, device_id={"pp": lax.rem(me + 1, n)}, device_id_type=MESH)

    pl.semaphore_wait(barrier, jnp.where(first, 0, 1) + jnp.where(last, 0, 1))

    for load in loads:
        load.wait()

    def prepare():
        for j in range(blocks):
            at = pl.ds(128 * j, 128)
            wgt[at, :] = wgu[:, pl.ds(256 * j, 128)].T
            wut[at, :] = wgu[:, pl.ds(256 * j + 128, 128)].T
            wdt[:, at] = wd[at, :].T
        accgu[...] = jnp.zeros_like(accgu)
        accd[...] = jnp.zeros_like(accd)

    def scaled(h):
        wide = h.astype(F32)
        scale = lax.rsqrt(jnp.mean(wide * wide, -1, keepdims=True) + 1e-6)
        return wide, scale, (wide * scale).astype(BF16)

    def forward(k):
        m, rows = rows_of(k)
        slot, hm = k % slots, m % hid_micros

        @pl.when(first)
        def _():
            x_copy(k).wait()

        @pl.when(me > 0)
        def _():
            h_copy(k).wait_recv()

        _, _, a = scaled(hbuf[m, rows, :])
        for j in range(blocks):
            both = dot(a, wgu[:, pl.ds(256 * j, 256)])
            gate, up = both[:, :128], both[:, 128:]
            s = jax.nn.sigmoid(gate)
            silu = gate * s
            at = pl.ds(128 * j, 128)
            pbuf[slot, :, at] = silu
            qbuf[slot, :, at] = up * (s + silu * (1.0 - s))
            hid[hm, rows, at] = (silu * up).astype(BF16)

        @pl.when(me < n - 1)
        def _():
            @pl.when(k >= OUT_SLOTS)
            def _():
                h_copy(k - OUT_SLOTS).wait_send()

            down = rounded(dot(hid[hm, rows, :], wd[...]))
            hout[k % OUT_SLOTS] = (hbuf[m, rows, :].astype(F32) + down).astype(BF16)
            h_copy(k).start()

    def backward(k):
        m, rows = rows_of(k)
        slot, two = k % slots, m % 2

        @pl.when(last)
        def _():
            dy_copy(k).wait()

        @pl.when(me < n - 1)
        def _():
            d_copy(k).wait_recv()

        dy = dbuf[m, rows, :]
        _, _, a = scaled(hbuf[m, rows, :])
        abuf[two, rows, :] = a
        for start in range(0, ff, 256):
            at = pl.ds(start, min(256, ff - start))
            dhid = rounded(dot(dy, wdt[:, at]))
            dgu[two, rows, at] = (dhid * qbuf[slot, :, at]).astype(BF16)
            dgu[two, rows, pl.ds(ff + start, min(256, ff - start))] = (dhid * pbuf[slot, :, at]).astype(BF16)

        @pl.when(me > 0)
        def _():
            @pl.when(k >= BACK_SLOTS)
            def _():
                d_copy(k - BACK_SLOTS).wait_send()

            by_gate = rounded(dot(dgu[two, rows, pl.ds(0, ff)], wgt[...]))
            by_up = rounded(dot(dgu[two, rows, pl.ds(ff, ff)], wut[...]))
            da = rounded(by_gate + by_up)
            wide, scale, _ = scaled(hbuf[m, rows, :])
            along = jnp.mean(da * wide, -1, keepdims=True)
            dn = rounded(da * scale - wide * (scale * scale * scale * along))
            dout[k % BACK_SLOTS] = (dbuf[m, rows, :].astype(F32) + dn).astype(BF16)
            d_copy(k).start()

    wide_tiles = 2 * ff // 256
    near = ff - 1024
    work = [
        [("gu", 256 * j, 256) for j in range(0, 4)],
        [("gu", 256 * j, 256) for j in range(4, 8)],
        [("gu", 256 * j, 256) for j in range(8, wide_tiles)] + [("d", 0, near)],
        [("d", near + 256 * i, 256) for i in range(4)],
    ]

    def weights(v):
        m, part = v // per, v % per
        two, hm = m % 2, m % hid_micros
        for number, items in enumerate(work):

            @pl.when(part == number)
            def _(items=items):
                for kind, start, size in items:
                    at = pl.ds(start, size)
                    if kind == "gu":
                        accgu[:, at] += rounded(dot_tokens(abuf[two], dgu[two, :, at]))
                    else:
                        accd[at, :] += rounded(dot_tokens(hid[hm, :, at], dbuf[m]))

    @pl.loop(0, chunks + lead + per)
    def _(t):
        @pl.when(t == jnp.where(first, lead, 0))
        def _():
            prepare()

        @pl.when(t < chunks)
        def _():
            forward(t)

        b = t - lead

        @pl.when((b >= 0) & (b < chunks))
        def _():
            backward(b)

        @pl.when(b >= per)
        def _():
            weights(b - per)

    outs = []

    def send_out(buffer, total, to):
        buffer[...] = total.astype(BF16)
        outs.append(pltpu.make_async_copy(buffer, to, o_sem.at[len(outs)]))
        outs[-1].start()

    for number, start in enumerate(range(0, ff, tokens)):
        at = pl.ds(start, min(tokens, ff - start))
        send_out(hbuf.at[number, pl.ds(0, at.size)], accd[at, :], od_ref.at[0, at])
    send_out(hid.at[0], accgu[:, pl.ds(0, ff)], og_ref.at[0])
    send_out(hid.at[1], accgu[:, pl.ds(ff, ff)], ou_ref.at[0])
    for copy in outs:
        copy.wait()

    @pl.when(me < n - 1)
    def _():
        @pl.loop(chunks - OUT_SLOTS, chunks)
        def _(k):
            h_copy(k).wait_send()

    @pl.when(me > 0)
    def _():
        @pl.loop(chunks - BACK_SLOTS, chunks)
        def _(k):
            d_copy(k).wait_send()


def solution(mesh):
    n = mesh.shape["pp"]

    def step(x, dy, w_gate, w_up, w_down):
        micro, tokens, dim = x.shape
        ff = w_down.shape[1]
        chunks = micro * (tokens // CHUNK)
        slots = (n - 1) * LEAD + 1
        any_space = pl.BlockSpec(memory_space=pl.ANY)
        return pl.pallas_call(
            functools.partial(kernel, n),
            out_shape=[jax.ShapeDtypeStruct(w.shape, BF16) for w in (w_gate, w_up, w_down)],
            in_specs=[any_space] * 5,
            out_specs=[any_space] * 3,
            scratch_shapes=[
                pltpu.VMEM((micro, tokens, dim), BF16),
                pltpu.VMEM((micro, tokens, dim), BF16),
                pltpu.VMEM((OUT_SLOTS, CHUNK, dim), BF16),
                pltpu.VMEM((BACK_SLOTS, CHUNK, dim), BF16),
                pltpu.VMEM((slots, CHUNK, ff), F32),
                pltpu.VMEM((slots, CHUNK, ff), F32),
                pltpu.VMEM((5, tokens, ff), BF16),
                pltpu.VMEM((2, tokens, 2 * ff), BF16),
                pltpu.VMEM((2, tokens, dim), BF16),
                pltpu.VMEM((dim, 2 * ff), BF16),
                pltpu.VMEM((ff, dim), BF16),
                pltpu.VMEM((ff, dim), BF16),
                pltpu.VMEM((ff, dim), BF16),
                pltpu.VMEM((dim, ff), BF16),
                pltpu.VMEM((dim, 2 * ff), F32),
                pltpu.VMEM((ff, dim), F32),
                pltpu.SemaphoreType.DMA((2 * (ff // 128) + 1,)),
                pltpu.SemaphoreType.DMA((chunks,)),
                pltpu.SemaphoreType.DMA((chunks,)),
                pltpu.SemaphoreType.DMA((chunks,)),
                pltpu.SemaphoreType.DMA((chunks,)),
                pltpu.SemaphoreType.DMA((-(-ff // tokens) + 2,)),
            ],
            compiler_params=pltpu.CompilerParams(collective_id=0, has_side_effects=True, vmem_limit_bytes=67_043_328),
        )(x, dy, w_gate, w_up, w_down)

    return jax.shard_map(
        step,
        mesh=mesh,
        in_specs=(P("rep", None, None),) * 2 + (P("pp", None, None),) * 3,
        out_specs=(P(("rep", "pp"), None, None),) * 3,
        check_vma=False,
    )
```

```python
import functools

import jax
import jax.numpy as jnp
from jax import lax
from jax.experimental import pallas as pl
from jax.experimental.pallas import tpu as pltpu
from jax.sharding import PartitionSpec as P

MESH = pl.DeviceIdType.MESH
F32, BF16 = jnp.float32, jnp.bfloat16
CHUNK = 128
HEAD, TAIL = (32, 32, 64), (64, 32, 32)
LEAD = 8
OUT_SLOTS, BACK_SLOTS = 16, 8


def dot(a, b):
    return jnp.dot(a, b, preferred_element_type=F32)


def dot_tokens(a, b):
    return lax.dot_general(a, b, (((0,), (0,)), ((), ())), preferred_element_type=F32)


def rounded(v):
    return v.astype(BF16).astype(F32)


def kernel(
    n, tokens, x_ref, dy_ref, wg_ref, wu_ref, wd_ref, og_ref, ou_ref, od_ref,
    hbuf, dbuf, hout, dout, pbuf, qbuf, hid, dgu, abuf, abuf_t, wgu, wd, wgt, wut, wdt, accgu, accd,
    w_sem, hrecv, drecv, hsend, dsend, o_sem,
):
    total, dim = x_ref.shape
    ff = wd_ref.shape[1]
    per = tokens // CHUNK
    heads, tails = len(HEAD), len(TAIL)
    units = total // CHUNK - 2 + heads + tails
    slots, hid_rows = pbuf.shape[0], hid.shape[0]
    blocks = ff // 128
    me = lax.axis_index("pp")
    first, last = me == 0, me == n - 1
    lead = ((n - 1 - me) * LEAD) // 2

    ends = [(k, sum(HEAD[:k]), size) for k, size in enumerate(HEAD)]
    ends += [(units - tails + k, total - CHUNK + sum(TAIL[:k]), size) for k, size in enumerate(TAIL)]

    def offset(k, size):
        off = (k - heads + 1) * CHUNK if size == CHUNK else 0
        for at, start, its in ends:
            if its == size:
                off = jnp.where(k == at, start, off)
        return pl.multiple_of(off, size)

    def is_size(k, size):
        if size == CHUNK:
            return (k >= heads) & (k < units - tails)
        found = False
        for at, _, its in ends:
            if its == size:
                found = (k == at) | found
        return found

    def per_size(k, body):
        for size in sorted({CHUNK, *HEAD, *TAIL}):

            @pl.when(is_size(k, size))
            def _(size=size):
                body(k, size, offset(k, size))

    def part_of(ref, off, size):
        return ref.at[pl.ds(pl.multiple_of(lax.rem(off, ref.shape[0]), size), size)]

    def x_copy(k, size, off):
        rows = pl.ds(off, size)
        return pltpu.make_async_copy(x_ref.at[rows], hbuf.at[rows], hrecv.at[k])

    def dy_copy(k, size, off):
        rows = pl.ds(off, size)
        return pltpu.make_async_copy(dy_ref.at[rows], dbuf.at[rows], drecv.at[k])

    def h_copy(k, size, off):
        return pltpu.make_async_remote_copy(
            src_ref=hout.at[lax.rem(k, OUT_SLOTS), pl.ds(0, size)], dst_ref=hbuf.at[pl.ds(off, size)],
            send_sem=hsend.at[k], recv_sem=hrecv.at[k], device_id={"pp": lax.rem(me + 1, n)}, device_id_type=MESH,
        )

    def d_copy(k, size, off):
        return pltpu.make_async_remote_copy(
            src_ref=dout.at[lax.rem(k, BACK_SLOTS), pl.ds(0, size)], dst_ref=dbuf.at[pl.ds(off, size)],
            send_sem=dsend.at[k], recv_sem=drecv.at[k], device_id={"pp": lax.rem(me + n - 1, n)}, device_id_type=MESH,
        )

    loads = []
    for j in range(blocks):
        for i, ref in enumerate((wg_ref, wu_ref)):
            to = wgu.at[:, pl.ds(256 * j + 128 * i, 128)]
            loads.append(pltpu.make_async_copy(ref.at[0, :, pl.ds(128 * j, 128)], to, w_sem.at[2 * j + i]))
    loads.append(pltpu.make_async_copy(wd_ref.at[0], wd, w_sem.at[2 * blocks]))

    barrier = pltpu.get_barrier_semaphore()

    @pl.when(me > 0)
    def _():
        pl.semaphore_signal(barrier, inc=1, device_id={"pp": lax.rem(me + n - 1, n)}, device_id_type=MESH)

    @pl.when(me < n - 1)
    def _():
        pl.semaphore_signal(barrier, inc=1, device_id={"pp": lax.rem(me + 1, n)}, device_id_type=MESH)

    @pl.when(first)
    def _():
        for at, start, size in ends[:heads]:
            x_copy(at, size, start).start()

    for load in loads:
        load.start()

    @pl.when(first)
    def _():
        @pl.loop(heads, units)
        def _(k):
            per_size(k, lambda *piece: x_copy(*piece).start())

    @pl.when(last)
    def _():
        @pl.loop(0, units)
        def _(k):
            per_size(k, lambda *piece: dy_copy(*piece).start())

    for load in loads:
        load.wait()
    pl.semaphore_wait(barrier, jnp.where(first, 0, 1) + jnp.where(last, 0, 1))

    def prepare():
        for j in range(blocks):
            at = pl.ds(128 * j, 128)
            wgt[at, :] = wgu[:, pl.ds(256 * j, 128)].T
            wut[at, :] = wgu[:, pl.ds(256 * j + 128, 128)].T
            wdt[:, at] = wd[at, :].T
        accgu[...] = jnp.zeros_like(accgu)
        accd[...] = jnp.zeros_like(accd)

    def scaled(h):
        wide = h.astype(F32)
        scale = lax.rsqrt(jnp.mean(wide * wide, -1, keepdims=True) + 1e-6)
        return wide, scale, (wide * scale).astype(BF16)

    def hidden(k, size, off):
        slot, hid_part = lax.rem(k, slots), part_of(hid, off, size)
        _, _, a = scaled(hbuf[pl.ds(off, size), :])
        for j in range(blocks):
            both = dot(a, wgu[:, pl.ds(256 * j, 256)])
            gate, up = both[:, :128], both[:, 128:]
            s = jax.nn.sigmoid(gate)
            silu = gate * s
            at = pl.ds(128 * j, 128)
            pbuf[slot, pl.ds(0, size), at] = silu
            qbuf[slot, pl.ds(0, size), at] = up * (s + silu * (1.0 - s))
            hid_part[:, at] = (silu * up).astype(BF16)

    def forward(k, size, off):
        @pl.when(first)
        def _():
            x_copy(k, size, off).wait()

        @pl.when(me > 0)
        def _():
            h_copy(k, size, off).wait_recv()

        @pl.when(k >= OUT_SLOTS)
        def _():
            per_size(k - OUT_SLOTS, lambda *piece: h_copy(*piece).wait_send())

        hidden(k, size, off)
        down = rounded(dot(part_of(hid, off, size)[...], wd[...]))
        hout[lax.rem(k, OUT_SLOTS), pl.ds(0, size), :] = (hbuf[pl.ds(off, size), :].astype(F32) + down).astype(BF16)
        h_copy(k, size, off).start()

    def backward_hidden(k, size, off):
        slot, rows, dgu_part = lax.rem(k, slots), pl.ds(off, size), part_of(dgu, off, size)
        dy = dbuf[rows, :]
        wide, scale, a = scaled(hbuf[rows, :])
        part_of(abuf, off, size)[...] = a
        for start in range(0, ff, 256):
            wide_by = min(256, ff - start)
            at = pl.ds(start, wide_by)
            dhid = rounded(dot(dy, wdt[:, at]))
            dgu_part[:, at] = (dhid * qbuf[slot, pl.ds(0, size), at]).astype(BF16)
            dgu_part[:, pl.ds(ff + start, wide_by)] = (dhid * pbuf[slot, pl.ds(0, size), at]).astype(BF16)
        return wide, scale

    def backward_input(k, size, off, wide, scale):
        dgu_part = part_of(dgu, off, size)
        by_gate = rounded(dot(dgu_part[:, pl.ds(0, ff)], wgt[...]))
        by_up = rounded(dot(dgu_part[:, pl.ds(ff, ff)], wut[...]))
        da = rounded(by_gate + by_up)
        along = jnp.mean(da * wide, -1, keepdims=True)
        dn = rounded(da * scale - wide * (scale * scale * scale * along))
        dout[lax.rem(k, BACK_SLOTS), pl.ds(0, size), :] = (dbuf[pl.ds(off, size), :].astype(F32) + dn).astype(BF16)
        d_copy(k, size, off).start()

    def back_slot_free(k):
        @pl.when(k >= BACK_SLOTS)
        def _():
            per_size(k - BACK_SLOTS, lambda *piece: d_copy(*piece).wait_send())

    def backward_first(k, size, off):
        d_copy(k, size, off).wait_recv()
        backward_hidden(k, size, off)

    def backward(k, size, off):
        d_copy(k, size, off).wait_recv()
        back_slot_free(k)
        backward_input(k, size, off, *backward_hidden(k, size, off))

    def forward_backward(k, size, off):
        dy_copy(k, size, off).wait()
        h_copy(k, size, off).wait_recv()
        back_slot_free(k)
        hidden(k, size, off)
        backward_input(k, size, off, *backward_hidden(k, size, off))

    down_near = 1024
    work = [
        [("d", 256 * i, 256) for i in range(down_near // 256)],
        [("d", down_near, ff - down_near)] + [("gu", 256 * j, 256) for j in range(0, 3)],
        [("gu", 256 * j, 256) for j in range(3, 7)],
        [("gu", 256 * j, 256) for j in range(7, 2 * ff // 256)],
    ]

    def weights(m, number, finish):
        two = pl.ds(pl.multiple_of(lax.rem(m, 2) * tokens, tokens), tokens)
        hid_at = pl.ds(pl.multiple_of(lax.rem(m * tokens, hid_rows), tokens), tokens)
        if number == 0:
            abuf_t[...] = abuf[two, :].T
        for kind, start, size in work[number]:
            at = pl.ds(start, size)
            if kind == "gu":
                term = rounded(dot(abuf_t[...], dgu[two, at]))
                ref, where = accgu, (slice(None), at)
            else:
                term = rounded(dot_tokens(hid[hid_at, at], dbuf[pl.ds(pl.multiple_of(m * tokens, tokens), tokens), :]))
                ref, where = accd, (at, slice(None))
            if finish is None:
                ref[where] += term
            else:
                finish(kind, start, size, ref[where] + term)

    @pl.loop(0, units + lead)
    def _(t):
        @pl.when(t == jnp.where(first, lead, 0))
        def _():
            prepare()

        @pl.when((t < units) & (me < n - 1))
        def _():
            per_size(t, forward)

        b = t - lead

        @pl.when((b >= 0) & first)
        def _():
            per_size(b, backward_first)

        @pl.when((b >= 0) & (me > 0) & (me < n - 1))
        def _():
            per_size(b, backward)

        @pl.when(last)
        def _():
            per_size(b, forward_backward)

        v = b - heads + 1 - per

        @pl.when((v >= 0) & (b <= units - tails))
        def _():
            for number in range(per):

                @pl.when(lax.rem(v, per) == number)
                def _(number=number):
                    weights(v // per, number, None)

    gate_out, up_out, down_out = hid.at[pl.ds(0, dim)], hid.at[pl.ds(dim, dim)], hbuf.at[pl.ds(0, ff)]
    outs = []

    def out(source, to):
        outs.append(pltpu.make_async_copy(source, to, o_sem.at[len(outs)]))
        outs[-1].start()

    def finish(kind, start, size, value):
        value = value.astype(BF16)
        if kind == "d":
            down_out[pl.ds(start, size), :] = value
            return
        for buffer, begin in ((gate_out, 0), (up_out, ff)):
            lo, hi = max(start, begin), min(start + size, begin + ff)
            if lo < hi:
                buffer[:, pl.ds(lo - begin, hi - lo)] = value[:, lo - start : hi - start]

    done = {"d": 0, "gu": 0}
    for number in range(per):
        weights(total // tokens - 1, number, finish)
        begun = dict(done)
        for kind, start, size in work[number]:
            done[kind] = start + size
        if done["d"] > begun["d"]:
            rows = pl.ds(begun["d"], done["d"] - begun["d"])
            out(down_out.at[rows], od_ref.at[0, rows])
        for buffer, to, begin in ((gate_out, og_ref, 0), (up_out, ou_ref, ff)):
            lo, hi = max(begun["gu"], begin), min(done["gu"], begin + ff)
            if lo < hi:
                columns = pl.ds(lo - begin, hi - lo)
                out(buffer.at[:, columns], to.at[0, :, columns])
    for copy in outs:
        copy.wait()

    @pl.when(me < n - 1)
    def _():
        @pl.loop(units - OUT_SLOTS, units)
        def _(k):
            per_size(k, lambda *piece: h_copy(*piece).wait_send())

    @pl.when(me > 0)
    def _():
        @pl.loop(units - BACK_SLOTS, units)
        def _(k):
            per_size(k, lambda *piece: d_copy(*piece).wait_send())


def copy_kernel(*refs):
    ins, outs, buffers, (in_sem, out_sem) = refs[:3], refs[3:6], refs[6:9], refs[9:]
    pieces = []
    for i, (source, to, buffer) in enumerate(zip(ins, outs, buffers, strict=True)):
        rows = source.shape[1] // 4
        for j in range(4):
            at = pl.ds(rows * j, rows)
            pieces.append((
                pltpu.make_async_copy(source.at[:, at], buffer.at[:, at], in_sem.at[4 * i + j]),
                pltpu.make_async_copy(buffer.at[:, at], to.at[:, at], out_sem.at[4 * i + j]),
            ))
    for come, _ in pieces:
        come.start()
    for come, go in pieces:
        come.wait()
        go.start()
    for _, go in pieces:
        go.wait()


def solution(mesh):
    n = mesh.shape["pp"]

    def step(x, dy, w_gate, w_up, w_down):
        micro, tokens, dim = x.shape
        ff = w_down.shape[1]
        total = micro * tokens
        units = total // CHUNK - 2 + len(HEAD) + len(TAIL)
        slots = (n - 1) * LEAD // 2 + 1
        any_space = pl.BlockSpec(memory_space=pl.ANY)
        shapes = [jax.ShapeDtypeStruct(w.shape, BF16) for w in (w_gate, w_up, w_down)]
        grads = pl.pallas_call(
            functools.partial(kernel, n, tokens),
            out_shape=shapes,
            in_specs=[any_space] * 5,
            out_specs=[any_space] * 3,
            scratch_shapes=[
                pltpu.VMEM((total, dim), BF16),
                pltpu.VMEM((total, dim), BF16),
                pltpu.VMEM((OUT_SLOTS, CHUNK, dim), BF16),
                pltpu.VMEM((BACK_SLOTS, CHUNK, dim), BF16),
                pltpu.VMEM((slots, CHUNK, ff), F32),
                pltpu.VMEM((slots, CHUNK, ff), F32),
                pltpu.VMEM((5 * tokens, ff), BF16),
                pltpu.VMEM((2 * tokens, 2 * ff), BF16),
                pltpu.VMEM((2 * tokens, dim), BF16),
                pltpu.VMEM((dim, tokens), BF16),
                pltpu.VMEM((dim, 2 * ff), BF16),
                pltpu.VMEM((ff, dim), BF16),
                pltpu.VMEM((ff, dim), BF16),
                pltpu.VMEM((ff, dim), BF16),
                pltpu.VMEM((dim, ff), BF16),
                pltpu.VMEM((dim, 2 * ff), F32),
                pltpu.VMEM((ff, dim), F32),
                pltpu.SemaphoreType.DMA((2 * (ff // 128) + 1,)),
                pltpu.SemaphoreType.DMA((units,)),
                pltpu.SemaphoreType.DMA((units,)),
                pltpu.SemaphoreType.DMA((units,)),
                pltpu.SemaphoreType.DMA((units,)),
                pltpu.SemaphoreType.DMA((8,)),
            ],
            compiler_params=pltpu.CompilerParams(collective_id=0, has_side_effects=True, vmem_limit_bytes=67_043_328),
        )(x.reshape(total, dim), dy.reshape(total, dim), w_gate, w_up, w_down)
        return pl.pallas_call(
            copy_kernel,
            out_shape=shapes,
            in_specs=[any_space] * 3,
            out_specs=[any_space] * 3,
            scratch_shapes=[pltpu.VMEM(s.shape, BF16) for s in shapes] + [pltpu.SemaphoreType.DMA((12,))] * 2,
            compiler_params=pltpu.CompilerParams(vmem_limit_bytes=67_043_328),
        )(*grads)

    return jax.shard_map(
        step,
        mesh=mesh,
        in_specs=(P("rep", None, None),) * 2 + (P("pp", None, None),) * 3,
        out_specs=(P(("rep", "pp"), None, None),) * 3,
        check_vma=False,
    )
```

```python
import functools

import jax
import jax.numpy as jnp
from jax import lax
from jax.experimental import pallas as pl
from jax.experimental.pallas import tpu as pltpu
from jax.sharding import PartitionSpec as P

MESH = pl.DeviceIdType.MESH
F32, BF16 = jnp.float32, jnp.bfloat16
CHUNK = 128
HALF = CHUNK // 2
LEAD = 8
OUT_SLOTS, BACK_SLOTS = 8, 8


def dot(a, b):
    return jnp.dot(a, b, preferred_element_type=F32)


def dot_tokens(a, b):
    return lax.dot_general(a, b, (((0,), (0,)), ((), ())), preferred_element_type=F32)


def rounded(v):
    return v.astype(BF16).astype(F32)


def kernel(
    n, tokens, x_ref, dy_ref, wg_ref, wu_ref, wd_ref, og_ref, ou_ref, od_ref,
    hbuf, dbuf, hout, dout, pbuf, qbuf, hid, dgu, abuf, abuf_t, wgu, wd, wgt, wut, wdt, accgu, accd,
    w_sem, hrecv, drecv, hsend, dsend,
):
    total, dim = x_ref.shape
    ff = wd_ref.shape[1]
    per = tokens // CHUNK
    units = total // CHUNK + 1
    slots, hid_rows = pbuf.shape[0], hid.shape[0]
    blocks = ff // 128
    me = lax.axis_index("pp")
    first, last = me == 0, me == n - 1
    lead = ((n - 1 - me) * LEAD) // 2

    early = lax.rem(lax.axis_index("rep"), 2) == 0
    other_half = jnp.where(early, 0, units - 2)

    def offset(k, size):
        if size == CHUNK:
            return pl.multiple_of(k * CHUNK - jnp.where(early, HALF, 0), HALF)
        return pl.multiple_of(jnp.where(k == units - 1, total - HALF, other_half * CHUNK), HALF)

    def per_size(k, body):
        is_half = (k == other_half) | (k == units - 1)

        @pl.when(is_half)
        def _():
            body(k, HALF, offset(k, HALF))

        @pl.when(jnp.logical_not(is_half))
        def _():
            body(k, CHUNK, offset(k, CHUNK))

    def ring(ref, off, size):
        return [ref.at[pl.ds(pl.multiple_of(lax.rem(off + at, ref.shape[0]), HALF), HALF)] for at in range(0, size, HALF)]

    def put(parts, columns, value):
        for number, part in enumerate(parts):
            part[:, columns] = value[HALF * number : HALF * (number + 1)]

    def get(parts, columns):
        return jnp.concatenate([part[:, columns] for part in parts], 0)

    def x_copy(k, size, off):
        rows = pl.ds(off, size)
        return pltpu.make_async_copy(x_ref.at[rows], hbuf.at[rows], hrecv.at[k])

    def dy_copy(k, size, off):
        rows = pl.ds(off, size)
        return pltpu.make_async_copy(dy_ref.at[rows], dbuf.at[rows], drecv.at[k])

    def h_copy(k, size, off):
        return pltpu.make_async_remote_copy(
            src_ref=hout.at[lax.rem(k, OUT_SLOTS), pl.ds(0, size)], dst_ref=hbuf.at[pl.ds(off, size)],
            send_sem=hsend.at[k], recv_sem=hrecv.at[k], device_id={"pp": lax.rem(me + 1, n)}, device_id_type=MESH,
        )

    def d_copy(k, size, off):
        return pltpu.make_async_remote_copy(
            src_ref=dout.at[lax.rem(k, BACK_SLOTS), pl.ds(0, size)], dst_ref=dbuf.at[pl.ds(off, size)],
            send_sem=dsend.at[k], recv_sem=drecv.at[k], device_id={"pp": lax.rem(me + n - 1, n)}, device_id_type=MESH,
        )

    loads = []
    for j in range(blocks):
        for i, ref in enumerate((wg_ref, wu_ref)):
            to = wgu.at[:, pl.ds(256 * j + 128 * i, 128)]
            loads.append(pltpu.make_async_copy(ref.at[0, :, pl.ds(128 * j, 128)], to, w_sem.at[2 * j + i]))
    loads.append(pltpu.make_async_copy(wd_ref.at[0], wd, w_sem.at[2 * blocks]))

    barrier = pltpu.get_barrier_semaphore()

    @pl.when(me > 0)
    def _():
        pl.semaphore_signal(barrier, inc=1, device_id={"pp": lax.rem(me + n - 1, n)}, device_id_type=MESH)

    @pl.when(me < n - 1)
    def _():
        pl.semaphore_signal(barrier, inc=1, device_id={"pp": lax.rem(me + 1, n)}, device_id_type=MESH)

    @pl.when(first)
    def _():
        per_size(0, lambda *piece: x_copy(*piece).start())

    for load in loads:
        load.start()

    @pl.when(first)
    def _():
        @pl.loop(1, units)
        def _(k):
            per_size(k, lambda *piece: x_copy(*piece).start())

    @pl.when(last)
    def _():
        @pl.loop(0, units)
        def _(k):
            per_size(k, lambda *piece: dy_copy(*piece).start())

    for load in loads:
        load.wait()
    pl.semaphore_wait(barrier, jnp.where(first, 0, 1) + jnp.where(last, 0, 1))

    def prepare():
        for j in range(blocks):
            at = pl.ds(128 * j, 128)
            wgt[at, :] = wgu[:, pl.ds(256 * j, 128)].T
            wut[at, :] = wgu[:, pl.ds(256 * j + 128, 128)].T
            wdt[:, at] = wd[at, :].T
        accgu[...] = jnp.zeros_like(accgu)
        accd[...] = jnp.zeros_like(accd)

    def scaled(h):
        wide = h.astype(F32)
        scale = lax.rsqrt(jnp.mean(wide * wide, -1, keepdims=True) + 1e-6)
        return wide, scale, (wide * scale).astype(BF16)

    def hidden(k, size, off):
        slot, hid_parts = lax.rem(k, slots), ring(hid, off, size)
        _, _, a = scaled(hbuf[pl.ds(off, size), :])
        for j in range(blocks):
            both = dot(a, wgu[:, pl.ds(256 * j, 256)])
            gate, up = both[:, :128], both[:, 128:]
            s = jax.nn.sigmoid(gate)
            silu = gate * s
            at = pl.ds(128 * j, 128)
            pbuf[slot, pl.ds(0, size), at] = silu
            qbuf[slot, pl.ds(0, size), at] = up * (s + silu * (1.0 - s))
            put(hid_parts, at, (silu * up).astype(BF16))

    def forward(k, size, off):
        @pl.when(first)
        def _():
            x_copy(k, size, off).wait()

        @pl.when(me > 0)
        def _():
            h_copy(k, size, off).wait_recv()

        @pl.when(k >= OUT_SLOTS)
        def _():
            per_size(k - OUT_SLOTS, lambda *piece: h_copy(*piece).wait_send())

        hidden(k, size, off)
        down = rounded(dot(get(ring(hid, off, size), pl.ds(0, ff)), wd[...]))
        hout[lax.rem(k, OUT_SLOTS), pl.ds(0, size), :] = (hbuf[pl.ds(off, size), :].astype(F32) + down).astype(BF16)
        h_copy(k, size, off).start()

    def backward_hidden(k, size, off):
        slot, rows, dgu_parts = lax.rem(k, slots), pl.ds(off, size), ring(dgu, off, size)
        dy = dbuf[rows, :]
        wide, scale, a = scaled(hbuf[rows, :])
        put(ring(abuf, off, size), pl.ds(0, dim), a)
        for start in range(0, ff, 256):
            wide_by = min(256, ff - start)
            at = pl.ds(start, wide_by)
            dhid = rounded(dot(dy, wdt[:, at]))
            put(dgu_parts, at, (dhid * qbuf[slot, pl.ds(0, size), at]).astype(BF16))
            put(dgu_parts, pl.ds(ff + start, wide_by), (dhid * pbuf[slot, pl.ds(0, size), at]).astype(BF16))
        return wide, scale

    def backward_input(k, size, off, wide, scale):
        dgu_parts = ring(dgu, off, size)
        by_gate = rounded(dot(get(dgu_parts, pl.ds(0, ff)), wgt[...]))
        by_up = rounded(dot(get(dgu_parts, pl.ds(ff, ff)), wut[...]))
        da = rounded(by_gate + by_up)
        along = jnp.mean(da * wide, -1, keepdims=True)
        dn = rounded(da * scale - wide * (scale * scale * scale * along))
        dout[lax.rem(k, BACK_SLOTS), pl.ds(0, size), :] = (dbuf[pl.ds(off, size), :].astype(F32) + dn).astype(BF16)
        d_copy(k, size, off).start()

    def back_slot_free(k):
        @pl.when(k >= BACK_SLOTS)
        def _():
            per_size(k - BACK_SLOTS, lambda *piece: d_copy(*piece).wait_send())

    def backward_first(k, size, off):
        d_copy(k, size, off).wait_recv()
        backward_hidden(k, size, off)

    def backward(k, size, off):
        d_copy(k, size, off).wait_recv()
        back_slot_free(k)
        backward_input(k, size, off, *backward_hidden(k, size, off))

    def forward_backward(k, size, off):
        dy_copy(k, size, off).wait()
        h_copy(k, size, off).wait_recv()
        back_slot_free(k)
        hidden(k, size, off)
        backward_input(k, size, off, *backward_hidden(k, size, off))

    down_near = 1024
    work = [
        [("d", 256 * i, 256) for i in range(down_near // 256)],
        [("d", down_near, ff - down_near)] + [("gu", 256 * j, 256) for j in range(0, 3)],
        [("gu", 256 * j, 256) for j in range(3, 7)],
        [("gu", 256 * j, 256) for j in range(7, 2 * ff // 256)],
    ]

    def weights(m, number, finish):
        two = pl.ds(pl.multiple_of(lax.rem(m, 2) * tokens, tokens), tokens)
        hid_at = pl.ds(pl.multiple_of(lax.rem(m * tokens, hid_rows), tokens), tokens)
        if number == 0:
            abuf_t[...] = abuf[two, :].T
        for kind, start, size in work[number]:
            at = pl.ds(start, size)
            if kind == "gu":
                term = rounded(dot(abuf_t[...], dgu[two, at]))
                ref, where = accgu, (slice(None), at)
            else:
                term = rounded(dot_tokens(hid[hid_at, at], dbuf[pl.ds(pl.multiple_of(m * tokens, tokens), tokens), :]))
                ref, where = accd, (at, slice(None))
            if finish is None:
                ref[where] += term
            else:
                finish(kind, start, size, ref[where] + term)

    @pl.loop(0, units + lead)
    def _(t):
        @pl.when(t == jnp.where(first, lead, 0))
        def _():
            prepare()

        @pl.when((t < units) & (me < n - 1))
        def _():
            per_size(t, forward)

        b = t - lead

        @pl.when((b >= 0) & first)
        def _():
            per_size(b, backward_first)

        @pl.when((b >= 0) & (me > 0) & (me < n - 1))
        def _():
            per_size(b, backward)

        @pl.when(last)
        def _():
            per_size(b, forward_backward)

        v = b - per

        @pl.when((v >= 0) & (b <= units - 2))
        def _():
            for number in range(per):

                @pl.when(lax.rem(v, per) == number)
                def _(number=number):
                    weights(v // per, number, None)

    def finish(kind, start, size, value):
        value = value.astype(BF16)
        if kind == "d":
            od_ref[0, pl.ds(start, size), :] = value
            return
        for ref, begin in ((og_ref, 0), (ou_ref, ff)):
            lo, hi = max(start, begin), min(start + size, begin + ff)
            if lo < hi:
                ref[0, :, pl.ds(lo - begin, hi - lo)] = value[:, lo - start : hi - start]

    for number in range(per):
        weights(total // tokens - 1, number, finish)

    @pl.when(me < n - 1)
    def _():
        @pl.loop(units - OUT_SLOTS, units)
        def _(k):
            per_size(k, lambda *piece: h_copy(*piece).wait_send())

    @pl.when(me > 0)
    def _():
        @pl.loop(units - BACK_SLOTS, units)
        def _(k):
            per_size(k, lambda *piece: d_copy(*piece).wait_send())


def copy_kernel(*refs):
    ins, outs, sem = refs[:3], refs[3:6], refs[6]
    copies = [pltpu.make_async_copy(source, to, sem.at[i]) for i, (source, to) in enumerate(zip(ins, outs, strict=True))]
    for copy in copies:
        copy.start()
    for copy in copies:
        copy.wait()


def solution(mesh):
    n = mesh.shape["pp"]

    def step(x, dy, w_gate, w_up, w_down):
        micro, tokens, dim = x.shape
        ff = w_down.shape[1]
        total = micro * tokens
        units = total // CHUNK + 1
        slots = (n - 1) * LEAD // 2 + 1
        any_space = pl.BlockSpec(memory_space=pl.ANY)
        shapes = [jax.ShapeDtypeStruct(w.shape, BF16) for w in (w_gate, w_up, w_down)]
        grads = pl.pallas_call(
            functools.partial(kernel, n, tokens),
            out_shape=[pltpu.VMEM(s.shape, BF16) for s in shapes],
            in_specs=[any_space] * 5,
            out_specs=[pl.BlockSpec(memory_space=pltpu.VMEM)] * 3,
            scratch_shapes=[
                pltpu.VMEM((total, dim), BF16),
                pltpu.VMEM((total, dim), BF16),
                pltpu.VMEM((OUT_SLOTS, CHUNK, dim), BF16),
                pltpu.VMEM((BACK_SLOTS, CHUNK, dim), BF16),
                pltpu.VMEM((slots, CHUNK, ff), F32),
                pltpu.VMEM((slots, CHUNK, ff), F32),
                pltpu.VMEM((5 * tokens, ff), BF16),
                pltpu.VMEM((2 * tokens, 2 * ff), BF16),
                pltpu.VMEM((2 * tokens, dim), BF16),
                pltpu.VMEM((dim, tokens), BF16),
                pltpu.VMEM((dim, 2 * ff), BF16),
                pltpu.VMEM((ff, dim), BF16),
                pltpu.VMEM((ff, dim), BF16),
                pltpu.VMEM((ff, dim), BF16),
                pltpu.VMEM((dim, ff), BF16),
                pltpu.VMEM((dim, 2 * ff), F32),
                pltpu.VMEM((ff, dim), F32),
                pltpu.SemaphoreType.DMA((2 * (ff // 128) + 1,)),
                pltpu.SemaphoreType.DMA((units,)),
                pltpu.SemaphoreType.DMA((units,)),
                pltpu.SemaphoreType.DMA((units,)),
                pltpu.SemaphoreType.DMA((units,)),
            ],
            compiler_params=pltpu.CompilerParams(collective_id=0, has_side_effects=True, vmem_limit_bytes=62_600_000),
        )(x.reshape(total, dim), dy.reshape(total, dim), w_gate, w_up, w_down)
        return pl.pallas_call(
            copy_kernel,
            out_shape=shapes,
            in_specs=[pl.BlockSpec(memory_space=pltpu.VMEM)] * 3,
            out_specs=[any_space] * 3,
            scratch_shapes=[pltpu.SemaphoreType.DMA((3,))],
            compiler_params=pltpu.CompilerParams(vmem_limit_bytes=1 << 20),
        )(*grads)

    return jax.shard_map(
        step,
        mesh=mesh,
        in_specs=(P("rep", None, None),) * 2 + (P("pp", None, None),) * 3,
        out_specs=(P(("rep", "pp"), None, None),) * 3,
        check_vma=False,
    )
```

```python
import functools

import jax
import jax.numpy as jnp
from jax import lax
from jax.experimental import pallas as pl
from jax.experimental.pallas import tpu as pltpu
from jax.sharding import PartitionSpec as P

MESH = pl.DeviceIdType.MESH
F32, BF16 = jnp.float32, jnp.bfloat16
VMEM = 67_043_328
CHUNK = 128
LEAD = 8
OUT_SLOTS, BACK_SLOTS = 8, 8
EXTRA = 0


def dot(a, b):
    return jnp.dot(a, b, preferred_element_type=F32)


def dot_tokens(a, b):
    return lax.dot_general(a, b, (((0,), (0,)), ((), ())), preferred_element_type=F32)


def rounded(v):
    return v.astype(BF16).astype(F32)


def weight_work(ff):
    near = 1024
    return [
        [("d", 256 * i, 256) for i in range(near // 256)],
        [("d", near, ff - near)] + [("gu", 256 * j, 256) for j in range(0, 3)],
        [("gu", 256 * j, 256) for j in range(3, 7)],
        [("gu", 256 * j, 256) for j in range(7, 2 * ff // 256)],
    ]


def weight_terms(m, items, turn, tokens, dbuf, hid, dgu, abuf, abuf_t, accgu, accd, finish):
    two = pl.ds(pl.multiple_of(lax.rem(m, 2) * tokens, tokens), tokens)
    hid_at = pl.ds(pl.multiple_of(lax.rem(m, hid.shape[0] // tokens) * tokens, tokens), tokens)
    if turn:
        abuf_t[...] = abuf[two, :].T
    for kind, start, size in items:
        at = pl.ds(start, size)
        if kind == "gu":
            term = rounded(dot(abuf_t[...], dgu[two, at]))
            ref, where = accgu, (slice(None), at)
        else:
            term = rounded(dot_tokens(hid[hid_at, at], dbuf[pl.ds(pl.multiple_of(m * tokens, tokens), tokens), :]))
            ref, where = accd, (at, slice(None))
        if finish is None:
            ref[where] += term
        else:
            finish(kind, start, size, ref[where] + term)


def kernel(
    n, tokens, x_ref, dy_ref, wg_ref, wu_ref, wd_ref, dbuf, hid, dgu, abuf, accgu, accd,
    hbuf, hout, dout, pbuf, qbuf, abuf_t, wgu, wd, wgt, wut, wdt,
    w_sem, hrecv, drecv, hsend, dsend,
):
    total, dim = x_ref.shape
    ff = wd_ref.shape[1]
    per = tokens // CHUNK
    units = total // CHUNK
    slots = pbuf.shape[0]
    blocks = ff // 128
    me = lax.axis_index("pp")
    first, last = me == 0, me == n - 1
    lead = ((n - 1 - me) * LEAD) // 2 + jnp.where(first, EXTRA, 0)

    def rows_of(k):
        return pl.ds(pl.multiple_of(k * CHUNK, CHUNK), CHUNK)

    def ring(ref, k):
        return ref.at[pl.ds(pl.multiple_of(lax.rem(k, ref.shape[0] // CHUNK) * CHUNK, CHUNK), CHUNK)]

    def x_copy(k):
        rows = rows_of(k)
        return pltpu.make_async_copy(x_ref.at[rows], hbuf.at[rows], hrecv.at[k])

    def dy_copy(k):
        rows = rows_of(k)
        return pltpu.make_async_copy(dy_ref.at[rows], dbuf.at[rows], drecv.at[k])

    def h_copy(k):
        return pltpu.make_async_remote_copy(
            src_ref=hout.at[lax.rem(k, OUT_SLOTS)], dst_ref=hbuf.at[rows_of(k)],
            send_sem=hsend.at[k], recv_sem=hrecv.at[k], device_id={"pp": lax.rem(me + 1, n)}, device_id_type=MESH,
        )

    def d_copy(k):
        return pltpu.make_async_remote_copy(
            src_ref=dout.at[lax.rem(k, BACK_SLOTS)], dst_ref=dbuf.at[rows_of(k)],
            send_sem=dsend.at[k], recv_sem=drecv.at[k], device_id={"pp": lax.rem(me + n - 1, n)}, device_id_type=MESH,
        )

    loads = []
    for j in range(blocks):
        for i, ref in enumerate((wg_ref, wu_ref)):
            to = wgu.at[:, pl.ds(256 * j + 128 * i, 128)]
            loads.append(pltpu.make_async_copy(ref.at[0, :, pl.ds(128 * j, 128)], to, w_sem.at[2 * j + i]))
    loads.append(pltpu.make_async_copy(wd_ref.at[0], wd, w_sem.at[2 * blocks]))

    barrier = pltpu.get_barrier_semaphore()

    @pl.when(me > 0)
    def _():
        pl.semaphore_signal(barrier, inc=1, device_id={"pp": lax.rem(me + n - 1, n)}, device_id_type=MESH)

    @pl.when(me < n - 1)
    def _():
        pl.semaphore_signal(barrier, inc=1, device_id={"pp": lax.rem(me + 1, n)}, device_id_type=MESH)

    @pl.when(first)
    def _():
        x_copy(0).start()

    for load in loads:
        load.start()

    @pl.when(first)
    def _():
        @pl.loop(1, units)
        def _(k):
            x_copy(k).start()

    @pl.when(last)
    def _():
        @pl.loop(0, units)
        def _(k):
            dy_copy(k).start()

    for load in loads:
        load.wait()
    pl.semaphore_wait(barrier, jnp.where(first, 0, 1) + jnp.where(last, 0, 1))

    def prepare():
        for j in range(blocks):
            at = pl.ds(128 * j, 128)
            wgt[at, :] = wgu[:, pl.ds(256 * j, 128)].T
            wut[at, :] = wgu[:, pl.ds(256 * j + 128, 128)].T
            wdt[:, at] = wd[at, :].T
        accgu[...] = jnp.zeros_like(accgu)
        accd[...] = jnp.zeros_like(accd)

    def scaled(h):
        wide = h.astype(F32)
        scale = lax.rsqrt(jnp.mean(wide * wide, -1, keepdims=True) + 1e-6)
        return wide, scale, (wide * scale).astype(BF16)

    def hidden(k):
        slot, hid_part = lax.rem(k, slots), ring(hid, k)
        _, _, a = scaled(hbuf[rows_of(k), :])
        for j in range(blocks):
            both = dot(a, wgu[:, pl.ds(256 * j, 256)])
            gate, up = both[:, :128], both[:, 128:]
            s = jax.nn.sigmoid(gate)
            silu = gate * s
            at = pl.ds(128 * j, 128)
            pbuf[slot, :, at] = silu
            qbuf[slot, :, at] = up * (s + silu * (1.0 - s))
            hid_part[:, at] = (silu * up).astype(BF16)

    def forward(k, after):
        hidden(k)
        down = rounded(dot(ring(hid, k)[...], wd[...]))
        hout[lax.rem(k, OUT_SLOTS)] = (hbuf[rows_of(k), :].astype(F32) + down).astype(BF16)
        h_copy(k).start()
        after()

    def backward_hidden(k):
        slot, rows, dgu_part = lax.rem(k, slots), rows_of(k), ring(dgu, k)
        dy = dbuf[rows, :]
        wide, scale, a = scaled(hbuf[rows, :])
        ring(abuf, k)[...] = a
        for start in range(0, ff, 256):
            wide_by = min(256, ff - start)
            at = pl.ds(start, wide_by)
            dhid = rounded(dot(dy, wdt[:, at]))
            dgu_part[:, at] = (dhid * qbuf[slot, :, at]).astype(BF16)
            dgu_part[:, pl.ds(ff + start, wide_by)] = (dhid * pbuf[slot, :, at]).astype(BF16)
        return wide, scale

    def backward_input(k, wide, scale):
        dgu_part = ring(dgu, k)
        by_gate = rounded(dot(dgu_part[:, pl.ds(0, ff)], wgt[...]))
        by_up = rounded(dot(dgu_part[:, pl.ds(ff, ff)], wut[...]))
        da = rounded(by_gate + by_up)
        along = jnp.mean(da * wide, -1, keepdims=True)
        dn = rounded(da * scale - wide * (scale * scale * scale * along))
        dout[lax.rem(k, BACK_SLOTS)] = (dbuf[rows_of(k), :].astype(F32) + dn).astype(BF16)
        d_copy(k).start()

    def back_slot_free(k):
        @pl.when(k >= BACK_SLOTS)
        def _():
            d_copy(k - BACK_SLOTS).wait_send()

    def backward(k):
        backward_input(k, *backward_hidden(k))

    def forward_backward(k, after):
        hidden(k)
        backward_input(k, *backward_hidden(k))
        after()

    work = weight_work(ff)

    def weights(m, number):
        weight_terms(m, work[number], number == 0, tokens, dbuf, hid, dgu, abuf, abuf_t, accgu, accd, None)

    def with_weights(b, body):
        @pl.when(b < per)
        def _():
            body(lambda: None)

        for number in range(per):

            @pl.when((b >= per) & (lax.rem(b, per) == number))
            def _(number=number):
                body(lambda: weights(b // per - 1, number))

    @pl.loop(0, units + lead)
    def _(t):
        b = t - lead

        @pl.when(t == jnp.where(first, lead, 0))
        def _():
            prepare()

        @pl.when((t < units) & (me < n - 1))
        def _():
            @pl.when(first)
            def _():
                x_copy(t).wait()

            @pl.when(me > 0)
            def _():
                h_copy(t).wait_recv()

            @pl.when(t >= OUT_SLOTS)
            def _():
                h_copy(t - OUT_SLOTS).wait_send()

            with_weights(b, lambda after: forward(t, after))

        @pl.when(t >= units)
        def _():
            with_weights(b, lambda after: after())

        @pl.when((b >= 0) & first)
        def _():
            d_copy(b).wait_recv()
            backward_hidden(b)

        @pl.when((b >= 0) & (me > 0) & (me < n - 1))
        def _():
            d_copy(b).wait_recv()
            back_slot_free(b)
            backward(b)

        @pl.when(last)
        def _():
            dy_copy(b).wait()
            h_copy(b).wait_recv()
            back_slot_free(b)
            with_weights(b, lambda after: forward_backward(b, after))

    @pl.when(me < n - 1)
    def _():
        @pl.loop(units - OUT_SLOTS, units)
        def _(k):
            h_copy(k).wait_send()

    @pl.when(me > 0)
    def _():
        @pl.loop(units - BACK_SLOTS, units)
        def _(k):
            d_copy(k).wait_send()


def finish_kernel(micro, tokens, dbuf, hid, dgu, abuf, accgu, accd, og_ref, ou_ref, od_ref, gate_out, up_out, down_out, abuf_t, sem):
    ff, dim = accd.shape
    outs = []

    def finish(kind, start, size, value):
        value = value.astype(BF16)
        if kind == "d":
            down_out[pl.ds(start, size), :] = value
            return
        for ref, begin in ((gate_out, 0), (up_out, ff)):
            lo, hi = max(start, begin), min(start + size, begin + ff)
            if lo < hi:
                ref[:, pl.ds(lo - begin, hi - lo)] = value[:, lo - start : hi - start]

    def out(source, to):
        outs.append(pltpu.make_async_copy(source, to, sem.at[len(outs)]))
        outs[-1].start()

    done = {"d": 0, "gu": 0}
    for number, items in enumerate(weight_work(ff)):
        weight_terms(micro - 1, items, number == 0, tokens, dbuf, hid, dgu, abuf, abuf_t, accgu, accd, finish)
        begun = dict(done)
        for kind, start, size in items:
            done[kind] = start + size
        if done["d"] > begun["d"]:
            rows = pl.ds(begun["d"], done["d"] - begun["d"])
            out(down_out.at[rows], od_ref.at[0, rows])
        for buffer, to, begin in ((gate_out, og_ref, 0), (up_out, ou_ref, ff)):
            lo, hi = max(begun["gu"], begin), min(done["gu"], begin + ff)
            if lo < hi:
                columns = pl.ds(lo - begin, hi - lo)
                out(buffer.at[:, columns], to.at[0, :, columns])
    for copy in outs:
        copy.wait()


def solution(mesh):
    n = mesh.shape["pp"]

    def step(x, dy, w_gate, w_up, w_down):
        micro, tokens, dim = x.shape
        ff = w_down.shape[1]
        total = micro * tokens
        units = total // CHUNK
        slots = (n - 1) * LEAD // 2 + EXTRA + 1
        hid_rows = -(-(slots + 7) * CHUNK // tokens) * tokens
        any_space, in_vmem = pl.BlockSpec(memory_space=pl.ANY), pl.BlockSpec(memory_space=pltpu.VMEM)
        left = [
            pltpu.VMEM((total, dim), BF16),
            pltpu.VMEM((hid_rows, ff), BF16),
            pltpu.VMEM((2 * tokens, 2 * ff), BF16),
            pltpu.VMEM((2 * tokens, dim), BF16),
            pltpu.VMEM((dim, 2 * ff), F32),
            pltpu.VMEM((ff, dim), F32),
        ]
        scratch = [
            pltpu.VMEM((total, dim), BF16),
            pltpu.VMEM((OUT_SLOTS, CHUNK, dim), BF16),
            pltpu.VMEM((BACK_SLOTS, CHUNK, dim), BF16),
            pltpu.VMEM((slots, CHUNK, ff), F32),
            pltpu.VMEM((slots, CHUNK, ff), F32),
            pltpu.VMEM((dim, tokens), BF16),
            pltpu.VMEM((dim, 2 * ff), BF16),
            pltpu.VMEM((ff, dim), BF16),
            pltpu.VMEM((ff, dim), BF16),
            pltpu.VMEM((ff, dim), BF16),
            pltpu.VMEM((dim, ff), BF16),
            pltpu.SemaphoreType.DMA((2 * (ff // 128) + 1,)),
        ] + [pltpu.SemaphoreType.DMA((units,))] * 4
        left_bytes = 2 * (total * dim + hid_rows * ff + 2 * tokens * (2 * ff + dim)) + 4 * 3 * ff * dim
        state = pl.pallas_call(
            functools.partial(kernel, n, tokens),
            out_shape=left,
            in_specs=[any_space] * 5,
            out_specs=[in_vmem] * len(left),
            scratch_shapes=scratch,
            compiler_params=pltpu.CompilerParams(
                collective_id=0, has_side_effects=True, vmem_limit_bytes=VMEM - left_bytes - (64 << 10)
            ),
        )(x.reshape(total, dim), dy.reshape(total, dim), w_gate, w_up, w_down)
        return pl.pallas_call(
            functools.partial(finish_kernel, micro, tokens),
            out_shape=[jax.ShapeDtypeStruct(w.shape, BF16) for w in (w_gate, w_up, w_down)],
            in_specs=[in_vmem] * len(left),
            out_specs=[any_space] * 3,
            scratch_shapes=[
                pltpu.VMEM((dim, ff), BF16),
                pltpu.VMEM((dim, ff), BF16),
                pltpu.VMEM((ff, dim), BF16),
                pltpu.VMEM((dim, tokens), BF16),
                pltpu.SemaphoreType.DMA((8,)),
            ],
            compiler_params=pltpu.CompilerParams(vmem_limit_bytes=8 << 20),
        )(*state)

    return jax.shard_map(
        step,
        mesh=mesh,
        in_specs=(P("rep", None, None),) * 2 + (P("pp", None, None),) * 3,
        out_specs=(P(("rep", "pp"), None, None),) * 3,
        check_vma=False,
    )
```

```python
import functools

import jax
import jax.numpy as jnp
from jax import lax
from jax.experimental import pallas as pl
from jax.experimental.pallas import tpu as pltpu
from jax.sharding import PartitionSpec as P

MESH = pl.DeviceIdType.MESH
F32, BF16 = jnp.float32, jnp.bfloat16
VMEM = 67_043_328
CHUNK = 128
LEAD = 8
OUT_SLOTS, BACK_SLOTS = 8, 8
EXTRA = 0


def dot(a, b):
    return jnp.dot(a, b, preferred_element_type=F32)


def dot_tokens(a, b):
    return lax.dot_general(a, b, (((0,), (0,)), ((), ())), preferred_element_type=F32)


def rounded(v):
    return v.astype(BF16).astype(F32)


def weight_work(ff):
    near = 1024
    return [
        [("d", 256 * i, 256) for i in range(near // 256)],
        [("d", near, ff - near)] + [("gu", 256 * j, 256) for j in range(0, 3)],
        [("gu", 256 * j, 256) for j in range(3, 7)],
        [("gu", 256 * j, 256) for j in range(7, 2 * ff // 256)],
    ]


def weight_terms(m, items, turn, tokens, dbuf, hid, dgu, abuf, abuf_t, accgu, accd, finish):
    two = pl.ds(pl.multiple_of(lax.rem(m, 2) * tokens, tokens), tokens)
    hid_at = pl.ds(pl.multiple_of(lax.rem(m, hid.shape[0] // tokens) * tokens, tokens), tokens)
    if turn:
        abuf_t[...] = abuf[two, :].T
    for kind, start, size in items:
        at = pl.ds(start, size)
        if kind == "gu":
            term = rounded(dot(abuf_t[...], dgu[two, at]))
            ref, where = accgu, (slice(None), at)
        else:
            term = rounded(dot_tokens(hid[hid_at, at], dbuf[pl.ds(pl.multiple_of(m * tokens, tokens), tokens), :]))
            ref, where = accd, (at, slice(None))
        if finish is None:
            ref[where] += term
        else:
            finish(kind, start, size, ref[where] + term)


def kernel(
    n, tokens, x_ref, dy_ref, wg_ref, wu_ref, wd_ref, dbuf, hid, dgu, abuf, accgu, accd,
    hbuf, hout, dout, pbuf, qbuf, dhid_buf, abuf_t, wgu, wd, wgt, wut, wdt,
    w_sem, hrecv, drecv, hsend, dsend,
):
    total, dim = x_ref.shape
    ff = wd_ref.shape[1]
    per = tokens // CHUNK
    units = total // CHUNK
    slots = pbuf.shape[0]
    blocks = ff // 128
    me = lax.axis_index("pp")
    first, last = me == 0, me == n - 1
    lead = ((n - 1 - me) * LEAD) // 2 + jnp.where(first, EXTRA, 0)

    def rows_of(k):
        return pl.ds(pl.multiple_of(k * CHUNK, CHUNK), CHUNK)

    def ring(ref, k):
        return ref.at[pl.ds(pl.multiple_of(lax.rem(k, ref.shape[0] // CHUNK) * CHUNK, CHUNK), CHUNK)]

    def x_copy(k):
        rows = rows_of(k)
        return pltpu.make_async_copy(x_ref.at[rows], hbuf.at[rows], hrecv.at[k])

    def dy_copy(k):
        rows = rows_of(k)
        return pltpu.make_async_copy(dy_ref.at[rows], dbuf.at[rows], drecv.at[k])

    def h_copy(k):
        return pltpu.make_async_remote_copy(
            src_ref=hout.at[lax.rem(k, OUT_SLOTS)], dst_ref=hbuf.at[rows_of(k)],
            send_sem=hsend.at[k], recv_sem=hrecv.at[k], device_id={"pp": lax.rem(me + 1, n)}, device_id_type=MESH,
        )

    def d_copy(k):
        return pltpu.make_async_remote_copy(
            src_ref=dout.at[lax.rem(k, BACK_SLOTS)], dst_ref=dbuf.at[rows_of(k)],
            send_sem=dsend.at[k], recv_sem=drecv.at[k], device_id={"pp": lax.rem(me + n - 1, n)}, device_id_type=MESH,
        )

    loads = []
    for j in range(blocks):
        for i, ref in enumerate((wg_ref, wu_ref)):
            to = wgu.at[:, pl.ds(256 * j + 128 * i, 128)]
            loads.append(pltpu.make_async_copy(ref.at[0, :, pl.ds(128 * j, 128)], to, w_sem.at[2 * j + i]))
    loads.append(pltpu.make_async_copy(wd_ref.at[0], wd, w_sem.at[2 * blocks]))

    barrier = pltpu.get_barrier_semaphore()

    @pl.when(me > 0)
    def _():
        pl.semaphore_signal(barrier, inc=1, device_id={"pp": lax.rem(me + n - 1, n)}, device_id_type=MESH)

    @pl.when(me < n - 1)
    def _():
        pl.semaphore_signal(barrier, inc=1, device_id={"pp": lax.rem(me + 1, n)}, device_id_type=MESH)

    @pl.when(first)
    def _():
        x_copy(0).start()

    for load in loads:
        load.start()

    @pl.when(first)
    def _():
        @pl.loop(1, units)
        def _(k):
            x_copy(k).start()

    @pl.when(last)
    def _():
        @pl.loop(0, units)
        def _(k):
            dy_copy(k).start()

    for load in loads[:-1]:
        load.wait()

    @pl.when(me > 0)
    def _():
        loads[-1].wait()

    pl.semaphore_wait(barrier, jnp.where(first, 0, 1) + jnp.where(last, 0, 1))

    def prepare():
        for j in range(blocks):
            at = pl.ds(128 * j, 128)
            wgt[at, :] = wgu[:, pl.ds(256 * j, 128)].T
            wut[at, :] = wgu[:, pl.ds(256 * j + 128, 128)].T
            wdt[:, at] = wd[at, :].T
        accgu[...] = jnp.zeros_like(accgu)
        accd[...] = jnp.zeros_like(accd)

    def scaled(h):
        wide = h.astype(F32)
        scale = lax.rsqrt(jnp.mean(wide * wide, -1, keepdims=True) + 1e-6)
        return wide, scale, (wide * scale).astype(BF16)

    def hidden(k):
        slot, hid_part = lax.rem(k, slots), ring(hid, k)
        _, _, a = scaled(hbuf[rows_of(k), :])
        for j in range(blocks):
            both = dot(a, wgu[:, pl.ds(256 * j, 256)])
            gate, up = both[:, :128], both[:, 128:]
            s = jax.nn.sigmoid(gate)
            silu = gate * s
            at = pl.ds(128 * j, 128)
            pbuf[slot, :, at] = silu
            qbuf[slot, :, at] = up * (s + silu * (1.0 - s))
            hid_part[:, at] = (silu * up).astype(BF16)

    def forward(k, after, load=None):
        hidden(k)
        if load:
            load.wait()
        down = rounded(dot(ring(hid, k)[...], wd[...]))
        hout[lax.rem(k, OUT_SLOTS)] = (hbuf[rows_of(k), :].astype(F32) + down).astype(BF16)
        h_copy(k).start()
        after()

    def backward_hidden(k, ready=False):
        slot, rows, dgu_part = lax.rem(k, slots), rows_of(k), ring(dgu, k)
        dy = dbuf[rows, :]
        wide, scale, a = scaled(hbuf[rows, :])
        ring(abuf, k)[...] = a
        for start in range(0, ff, 256):
            wide_by = min(256, ff - start)
            at = pl.ds(start, wide_by)
            dhid = dhid_buf[:, at].astype(F32) if ready else rounded(dot(dy, wdt[:, at]))
            dgu_part[:, at] = (dhid * qbuf[slot, :, at]).astype(BF16)
            dgu_part[:, pl.ds(ff + start, wide_by)] = (dhid * pbuf[slot, :, at]).astype(BF16)
        return wide, scale

    def backward_input(k, wide, scale):
        dgu_part = ring(dgu, k)
        by_gate = rounded(dot(dgu_part[:, pl.ds(0, ff)], wgt[...]))
        by_up = rounded(dot(dgu_part[:, pl.ds(ff, ff)], wut[...]))
        da = rounded(by_gate + by_up)
        along = jnp.mean(da * wide, -1, keepdims=True)
        dn = rounded(da * scale - wide * (scale * scale * scale * along))
        dout[lax.rem(k, BACK_SLOTS)] = (dbuf[rows_of(k), :].astype(F32) + dn).astype(BF16)
        d_copy(k).start()

    def back_slot_free(k):
        @pl.when(k >= BACK_SLOTS)
        def _():
            d_copy(k - BACK_SLOTS).wait_send()

    def backward(k):
        backward_input(k, *backward_hidden(k))

    def forward_backward(k, after):
        hidden(k)
        backward_input(k, *backward_hidden(k, ready=True))
        after()

    work = weight_work(ff)

    def weights(m, number):
        weight_terms(m, work[number], number == 0, tokens, dbuf, hid, dgu, abuf, abuf_t, accgu, accd, None)

    def with_weights(b, body):
        @pl.when(b < per)
        def _():
            body(lambda: None)

        for number in range(per):

            @pl.when((b >= per) & (lax.rem(b, per) == number))
            def _(number=number):
                body(lambda: weights(b // per - 1, number))

    @pl.loop(0, units + lead)
    def _(t):
        b = t - lead

        @pl.when(t == jnp.where(first, lead, 0))
        def _():
            prepare()

        @pl.when((t < units) & (me < n - 1))
        def _():
            @pl.when(first)
            def _():
                x_copy(t).wait()

            @pl.when(me > 0)
            def _():
                h_copy(t).wait_recv()

            @pl.when(t >= OUT_SLOTS)
            def _():
                h_copy(t - OUT_SLOTS).wait_send()

            @pl.when(first & (t == 0))
            def _():
                forward(t, lambda: None, loads[-1])

            @pl.when((me > 0) | (t > 0))
            def _():
                with_weights(b, lambda after: forward(t, after))

        @pl.when(t >= units)
        def _():
            with_weights(b, lambda after: after())

        @pl.when((b >= 0) & first)
        def _():
            d_copy(b).wait_recv()
            backward_hidden(b)

        @pl.when((b >= 0) & (me > 0) & (me < n - 1))
        def _():
            d_copy(b).wait_recv()
            back_slot_free(b)
            backward(b)

        @pl.when(last)
        def _():
            dy_copy(b).wait()
            back_slot_free(b)
            dhid_buf[...] = dot(dbuf[rows_of(b), :], wdt[...]).astype(BF16)
            h_copy(b).wait_recv()
            with_weights(b, lambda after: forward_backward(b, after))

    @pl.when(me < n - 1)
    def _():
        @pl.loop(units - OUT_SLOTS, units)
        def _(k):
            h_copy(k).wait_send()

    @pl.when(me > 0)
    def _():
        @pl.loop(units - BACK_SLOTS, units)
        def _(k):
            d_copy(k).wait_send()


def finish_kernel(micro, tokens, dbuf, hid, dgu, abuf, accgu, accd, og_ref, ou_ref, od_ref, gate_out, up_out, down_out, abuf_t, sem):
    ff, dim = accd.shape
    outs = []

    def finish(kind, start, size, value):
        value = value.astype(BF16)
        if kind == "d":
            down_out[pl.ds(start, size), :] = value
            return
        for ref, begin in ((gate_out, 0), (up_out, ff)):
            lo, hi = max(start, begin), min(start + size, begin + ff)
            if lo < hi:
                ref[:, pl.ds(lo - begin, hi - lo)] = value[:, lo - start : hi - start]

    def out(source, to):
        outs.append(pltpu.make_async_copy(source, to, sem.at[len(outs)]))
        outs[-1].start()

    done = {"d": 0, "gu": 0}
    near, *rest = weight_work(ff)
    wide = [item for part in rest for item in part if item[0] == "gu"]
    narrow = [item for part in rest for item in part if item[0] == "d"]
    for number, items in enumerate([near, wide[:4], wide[4:8], wide[8:], narrow]):
        weight_terms(micro - 1, items, number == 0, tokens, dbuf, hid, dgu, abuf, abuf_t, accgu, accd, finish)
        begun = dict(done)
        for kind, start, size in items:
            done[kind] = start + size
        if done["d"] > begun["d"]:
            rows = pl.ds(begun["d"], done["d"] - begun["d"])
            out(down_out.at[rows], od_ref.at[0, rows])
        for buffer, to, begin in ((gate_out, og_ref, 0), (up_out, ou_ref, ff)):
            lo, hi = max(begun["gu"], begin), min(done["gu"], begin + ff)
            if lo < hi:
                columns = pl.ds(lo - begin, hi - lo)
                out(buffer.at[:, columns], to.at[0, :, columns])
    for copy in outs:
        copy.wait()


def solution(mesh):
    n = mesh.shape["pp"]

    def step(x, dy, w_gate, w_up, w_down):
        micro, tokens, dim = x.shape
        ff = w_down.shape[1]
        total = micro * tokens
        units = total // CHUNK
        slots = (n - 1) * LEAD // 2 + EXTRA + 1
        hid_rows = -(-(slots + 7) * CHUNK // tokens) * tokens
        any_space, in_vmem = pl.BlockSpec(memory_space=pl.ANY), pl.BlockSpec(memory_space=pltpu.VMEM)
        left = [
            pltpu.VMEM((total, dim), BF16),
            pltpu.VMEM((hid_rows, ff), BF16),
            pltpu.VMEM((2 * tokens, 2 * ff), BF16),
            pltpu.VMEM((2 * tokens, dim), BF16),
            pltpu.VMEM((dim, 2 * ff), F32),
            pltpu.VMEM((ff, dim), F32),
        ]
        scratch = [
            pltpu.VMEM((total, dim), BF16),
            pltpu.VMEM((OUT_SLOTS, CHUNK, dim), BF16),
            pltpu.VMEM((BACK_SLOTS, CHUNK, dim), BF16),
            pltpu.VMEM((slots, CHUNK, ff), F32),
            pltpu.VMEM((slots, CHUNK, ff), F32),
            pltpu.VMEM((CHUNK, ff), BF16),
            pltpu.VMEM((dim, tokens), BF16),
            pltpu.VMEM((dim, 2 * ff), BF16),
            pltpu.VMEM((ff, dim), BF16),
            pltpu.VMEM((ff, dim), BF16),
            pltpu.VMEM((ff, dim), BF16),
            pltpu.VMEM((dim, ff), BF16),
            pltpu.SemaphoreType.DMA((2 * (ff // 128) + 1,)),
        ] + [pltpu.SemaphoreType.DMA((units,))] * 4
        left_bytes = 2 * (total * dim + hid_rows * ff + 2 * tokens * (2 * ff + dim)) + 4 * 3 * ff * dim
        state = pl.pallas_call(
            functools.partial(kernel, n, tokens),
            out_shape=left,
            in_specs=[any_space] * 5,
            out_specs=[in_vmem] * len(left),
            scratch_shapes=scratch,
            compiler_params=pltpu.CompilerParams(
                collective_id=0, has_side_effects=True, vmem_limit_bytes=VMEM - left_bytes - (64 << 10)
            ),
        )(x.reshape(total, dim), dy.reshape(total, dim), w_gate, w_up, w_down)
        return pl.pallas_call(
            functools.partial(finish_kernel, micro, tokens),
            out_shape=[jax.ShapeDtypeStruct(w.shape, BF16) for w in (w_gate, w_up, w_down)],
            in_specs=[in_vmem] * len(left),
            out_specs=[any_space] * 3,
            scratch_shapes=[
                pltpu.VMEM((dim, ff), BF16),
                pltpu.VMEM((dim, ff), BF16),
                pltpu.VMEM((ff, dim), BF16),
                pltpu.VMEM((dim, tokens), BF16),
                pltpu.SemaphoreType.DMA((8,)),
            ],
            compiler_params=pltpu.CompilerParams(vmem_limit_bytes=8 << 20),
        )(*state)

    return jax.shard_map(
        step,
        mesh=mesh,
        in_specs=(P("rep", None, None),) * 2 + (P("pp", None, None),) * 3,
        out_specs=(P(("rep", "pp"), None, None),) * 3,
        check_vma=False,
    )
```
